32 devices in a mesh: src: 4 (over z), rcv: 8 (over y, x, core).
Axes of the slice: x: 2, y: 2, z: 4, core: 2. Of those that a mesh axis runs over, the one named last changes fastest.
Arguments:
- traces: bfloat16 [512, 2048, 512], P('src', 'rcv'), may hold values from -6 to 6
- virtual_source_index: int32 [256], replicated, may hold values from 0 to 2047
Outputs:
- correlations: float32 [256, 2048, 512], P('rcv', 'src')
The draws below stay inside these ranges and needn't reach their ends.
Inputs may be any that keep to these rules, and one draw needn't show every extreme that they name: `virtual_source_index`: receiver numbers; a receiver may be listed more than once.
All inputs are finite; a program needn't handle non-finite values.
Results may differ from the reference program's by a relative error of at most 0.0064.
Values may be sent and summed in bfloat16 or wider, within the bound.
A program may use at most 192 MiB of HBM per device.

```python
import math
import jax
import jax.numpy as jnp
from jax import lax

NT = 512
NF = 128
RCV = 2048
VS = 256
SHOTS = 512


def place_ends(array, stream_key, smallest, top_value):
    dims = array.shape
    place = [jax.random.randint(jax.random.fold_in(stream_key, axis), (), 0, dims[axis]) for axis in range(len(dims))]
    array = array.at[tuple(place)].set(smallest)
    longest = dims.index(max(dims))
    place[longest] = (place[longest] + 1) % dims[longest]
    return array.at[tuple(place)].set(top_value)


def shard_levels(key, dims, pieces, least, high):
    loudness = 1.0
    for position, shards_of in pieces:
        steps = jax.random.uniform(jax.random.fold_in(jax.random.fold_in(key, 6), position), (shards_of,), jnp.float32, least / len(pieces), high / len(pieces))
        loudness = loudness * jnp.repeat(jnp.exp(steps), dims[position] // shards_of).reshape((-1,) + (1,) * (len(dims) - 1 - position))
    return loudness


def noise(own_key, shape, width, most, split=(), kind=jnp.bfloat16):
    entries = jax.random.normal(own_key, shape, jnp.float32) * width
    if len(split) > 0:
        entries = shard_levels(own_key, shape, split, -0.22, 0.18) * entries
    return jnp.clip(entries, min=-most, max=most).astype(kind)


def setup_inputs(seed: int = 0) -> dict:
    streams_of = jax.random.split(jax.random.key(seed), 3)
    return {
        "traces": noise(streams_of[0], (SHOTS, RCV, NT), 1.0, 6.0, ((0, 4), (1, 8))),
        "virtual_source_index": place_ends(jax.random.randint(streams_of[1], (VS,), 0, RCV), jax.random.fold_in(streams_of[1], 1), 0, RCV - 1).astype(jnp.int32),
    }


def make_tables():
    freqs = jnp.arange(NF, dtype=jnp.int32)
    times = jnp.arange(NT, dtype=jnp.int32)
    phase = (freqs[:, None] * times[None, :] % NT).astype(jnp.float32) * (2.0 * math.pi / NT)
    basis = jnp.stack([jnp.cos(phase), -jnp.sin(phase)], axis=1)
    forward = (basis / jnp.sqrt(jnp.float32(NT))).astype(jnp.bfloat16)
    inverse = (basis / jnp.sqrt(jnp.float32(NF))).astype(jnp.bfloat16)
    return (forward, inverse)

def complex_gram(left_operand, right_operand):
    high_precision = lax.Precision.HIGHEST
    real_part = jnp.einsum('ekg,ekh->egh', left_operand[:, 0], right_operand[:, 0], precision=high_precision) + jnp.einsum('ekg,ekh->egh', left_operand[:, 1], right_operand[:, 1], precision=high_precision)
    imaginary_part = jnp.einsum('ekg,ekh->egh', left_operand[:, 0], right_operand[:, 1], precision=high_precision) - jnp.einsum('ekg,ekh->egh', left_operand[:, 1], right_operand[:, 0], precision=high_precision)
    return jnp.stack([real_part, imaginary_part], axis=1)

def reference(traces, virtual_source_index):
    forward, inverse = make_tables()
    frequency_block = 8
    flat = traces.reshape(SHOTS * RCV, NT)
    scale = 1.0 / jnp.sqrt(jnp.float32(SHOTS))

    def one_block(table):
        spec = jnp.dot(flat, table.reshape(frequency_block * 2, NT).T, preferred_element_type=jnp.float32)
        spec = spec.astype(jnp.bfloat16).reshape(SHOTS, RCV, frequency_block, 2).transpose(2, 3, 0, 1).astype(jnp.float32)
        rows = jnp.take(spec, virtual_source_index, axis=3)
        gram = complex_gram(rows, spec) * scale
        return gram.astype(jnp.bfloat16)
    scaled = lax.map(one_block, forward.reshape(NF // frequency_block, frequency_block, 2, NT))
    scaled = scaled.reshape(NF, 2, VS, RCV).transpose(2, 0, 1, 3)
    inverse_flattened = inverse.reshape(2 * NF, NT)

    def one_source(block):
        return jnp.dot(block.reshape(2 * NF, RCV).T, inverse_flattened, preferred_element_type=jnp.float32)
    return lax.map(one_source, scaled)
```

```python
import functools
import math

import jax
import jax.numpy as jnp
from jax import lax
from jax.experimental import pallas as pl
from jax.sharding import PartitionSpec as P


NF = 128
CHUNKS = 4


def make_tables(times_count):
    freqs = jnp.arange(NF, dtype=jnp.int32)
    times = jnp.arange(times_count, dtype=jnp.int32)
    phase = (freqs[:, None] * times[None, :] % times_count).astype(jnp.float32) * (
        2.0 * math.pi / times_count
    )
    basis = jnp.stack([jnp.cos(phase), -jnp.sin(phase)], axis=1)
    forward = (basis / jnp.sqrt(jnp.float32(times_count))).astype(jnp.bfloat16)
    inverse = (basis / jnp.sqrt(jnp.float32(NF))).astype(jnp.bfloat16)
    return (forward, inverse)


def rows_kernel(spectra_ref, pick_ref, rows_ref):
    owners, _, _, shots, receivers = spectra_ref.shape
    total = None
    for owner in range(owners):
        part = jnp.dot(
            spectra_ref[owner, 0].reshape(2 * shots, receivers),
            pick_ref[owner],
            preferred_element_type=jnp.float32,
        )
        total = part if total is None else total + part
    rows_ref[0] = total.astype(rows_ref.dtype).reshape(rows_ref.shape[1:])


def pick_rows(spectra, pick):
    owners, freqs, _, shots, receivers = spectra.shape
    sources = pick.shape[2]
    return pl.pallas_call(
        rows_kernel,
        grid=(freqs,),
        in_specs=[
            pl.BlockSpec((owners, 1, 2, shots, receivers), lambda f: (0, f, 0, 0, 0)),
            pl.BlockSpec((owners, receivers, sources), lambda f: (0, 0, 0)),
        ],
        out_specs=pl.BlockSpec((1, 2, shots, sources), lambda f: (f, 0, 0, 0)),
        out_shape=jax.ShapeDtypeStruct((freqs, 2, shots, sources), jnp.bfloat16),
        cost_estimate=pl.CostEstimate(
            flops=4 * freqs * shots * owners * receivers * sources,
            bytes_accessed=spectra.size * 2 + pick.size * 2,
            transcendentals=0,
        ),
    )(spectra, pick)


def gram_kernel(scale, groups, *refs):
    rows_refs, columns_refs, out_ref = refs[:groups], refs[groups:-1], refs[-1]
    _, _, shots, sources = rows_refs[0].shape
    blocks, receivers = columns_refs[0].shape[0], columns_refs[0].shape[4]
    rows = [rows_ref[0] for rows_ref in rows_refs]
    real_left = jnp.concatenate([row.reshape(2 * shots, sources) for row in rows], axis=0)
    imaginary_left = jnp.concatenate(
        [piece for row in rows for piece in (-row[1], row[0])], axis=0
    )
    owners, _, _, own, _ = out_ref.shape
    for block in range(blocks):
        right = jnp.concatenate(
            [
                columns_ref[block, 0].reshape(2 * shots, receivers)
                for columns_ref in columns_refs
            ],
            axis=0,
        )
        for part, left in enumerate((real_left, imaginary_left)):
            gram = lax.dot_general(
                left, right, (((0,), (0,)), ((), ())), preferred_element_type=jnp.float32
            )
            out_ref[:, 0, part, :, block * receivers : (block + 1) * receivers] = (
                (gram * scale).astype(out_ref.dtype).reshape(owners, own, receivers)
            )


def scaled_gram(rows, columns, owners):
    groups = len(rows)
    freqs, _, shots, sources = rows[0].shape
    blocks, receivers = columns[0].shape[0], columns[0].shape[4]
    own = sources // owners
    scale = 1.0 / math.sqrt(groups * shots)
    return pl.pallas_call(
        functools.partial(gram_kernel, scale, groups),
        grid=(freqs,),
        in_specs=[pl.BlockSpec((1, 2, shots, sources), lambda f: (f, 0, 0, 0))] * groups
        + [pl.BlockSpec((blocks, 1, 2, shots, receivers), lambda f: (0, f, 0, 0, 0))]
        * groups,
        out_specs=pl.BlockSpec(
            (owners, 1, 2, own, blocks * receivers), lambda f: (0, f, 0, 0, 0)
        ),
        out_shape=jax.ShapeDtypeStruct(
            (owners, freqs, 2, own, blocks * receivers), jnp.bfloat16
        ),
        cost_estimate=pl.CostEstimate(
            flops=8 * freqs * groups * shots * sources * blocks * receivers,
            bytes_accessed=groups * (rows[0].size + columns[0].size) * 2,
            transcendentals=0,
        ),
    )(*rows, *columns)


def shifted(array, shift, count):
    return lax.ppermute(array, "src", [(i, (i + shift) % count) for i in range(count)])


def shards(traces, virtual_source_index):
    shots_here, rcv_here, times_count = traces.shape
    n_src, n_rcv = lax.axis_size("src"), lax.axis_size("rcv")
    me = lax.axis_index("src")
    sources = virtual_source_index.shape[0]
    forward, inverse = make_tables(times_count)
    chunks = CHUNKS
    per = NF // n_rcv // chunks
    forward = forward.reshape(n_rcv, chunks, per, 2, times_count)
    inverse = inverse.reshape(n_rcv, chunks, per, 2, times_count)
    receivers = jnp.arange(n_rcv * rcv_here, dtype=jnp.int32)
    pick = (receivers[:, None] == virtual_source_index[None, :]).astype(jnp.bfloat16)
    pick = pick.reshape(n_rcv, rcv_here, sources)
    blocks = n_rcv // n_src
    folded = []
    for chunk in range(chunks):
        spectra = jnp.einsum(
            "kt,srt->ksr",
            forward[:, chunk].reshape(n_rcv * per * 2, times_count),
            traces,
            preferred_element_type=jnp.float32,
        )
        spectra = spectra.astype(jnp.bfloat16)
        spectra = spectra.reshape(n_rcv, per, 2, shots_here, rcv_here)
        spectra = lax.all_to_all(
            spectra, "rcv", split_axis=0, concat_axis=0, tiled=True
        )
        columns = spectra.reshape(n_src, blocks, per, 2, shots_here, rcv_here)
        pieces = []
        for shift in range(n_src):
            target = lax.rem(me + shift, n_src)
            piece = lax.dynamic_index_in_dim(columns, target, 0, keepdims=False)
            pieces.append(shifted(piece, shift, n_src) if shift else piece)
        rows = pick_rows(spectra, pick)
        rows = [shifted(rows, shift, n_src) if shift else rows for shift in range(n_src)]
        scaled = scaled_gram(rows, pieces, n_rcv)
        folded.append(
            lax.all_to_all(scaled, "rcv", split_axis=0, concat_axis=0, tiled=True)
        )
    folded = jnp.stack(folded, axis=1)
    folded = folded.reshape(NF * 2, folded.shape[4], folded.shape[5])
    return jnp.einsum(
        "kt,kvr->vrt",
        inverse.reshape(NF * 2, times_count),
        folded,
        preferred_element_type=jnp.float32,
    )


def solution(mesh):
    placed = (P("src", "rcv", None), P())

    return jax.shard_map(
        shards, mesh=mesh, in_specs=placed, out_specs=P("rcv", "src", None), check_vma=False
    )
```
